128 devices in a mesh: row: 16 (over y, x), col: 4 (over z), depth: 2 (over core).
Axes of the slice: x: 4, y: 4, z: 4, core: 2. Of those that a mesh axis runs over, the one named last changes fastest.
Arguments:
- layers: float32 [2, 16384, 16384], P('depth', 'row', 'col'), may hold values from -3 to 265.4, as said below
Outputs:
- factor: float32 [2, 16384, 512], P(None, 'row', 'depth')
- schur: float32 [16384, 16384], P(('row', 'depth'), 'col')
The draws below stay inside these ranges and needn't reach their ends.
Inputs may be any that keep to these rules, and one draw needn't show every extreme that they name: Read in matrix order, each layer is symmetric, and the sum over layers is symmetric positive definite with a diagonal of order sqrt(16384).
All inputs are finite; a program needn't handle non-finite values.
Results may differ from the reference program's by a relative error of at most 0.0001.
Values sent between devices are 32-bit elements; how exact they have to be, the bound alone decides.
No kernel may reach another device: no remote copies, remote signals or barrier semaphores. Data moves between devices by JAX's collectives and lax.ppermute only.
A program may use at most 192 MiB of HBM per device.

```python
import jax
import jax.numpy as jnp
from jax import lax

PANEL = 512
BLOCKS_DEV = 2
PANELS = 2
LAYERS = 2
ORDER = 16384
COL_BLOCKS = 8
N_ROW = 16
N_COL = 4


def draw_layers(key, part):
    row_groups = ORDER // (PANEL * BLOCKS_DEV)
    col_groups = ORDER // (PANEL * COL_BLOCKS)
    positions = jnp.arange(ORDER, dtype=jnp.float32)
    distance = jnp.abs(positions[:, None] - positions[None, :])

    def one_layer(layer_index):
        layer_key = jax.random.fold_in(key, layer_index)
        noise_key, diag_key, scale_key, amp_key, reach_key = jax.random.split(layer_key, 5)
        noise = jnp.clip(jax.random.normal(noise_key, (ORDER, ORDER), jnp.float32), -4.0, 4.0)
        reach = PANEL * jax.random.uniform(reach_key, (), jnp.float32, 0.04, 0.12)
        amplitude = ORDER ** 0.5 * jax.random.uniform(amp_key, (), jnp.float32, 0.2, 0.45)
        symmetric = (noise + noise.T) * (0.5 / 1.4142135)
        row_scale = jax.random.uniform(scale_key, (ORDER,), jnp.float32, 0.7, 1.3)
        kernel = amplitude * row_scale[:, None] * row_scale[None, :] * jnp.exp(-distance / reach)
        diag_values = ORDER ** 0.5 * jax.random.uniform(diag_key, (ORDER,), jnp.float32, 0.75, 1.25)
        matrix = symmetric + kernel + jnp.diag(diag_values)
        rows = matrix.reshape(BLOCKS_DEV, row_groups, PANEL, ORDER).transpose(1, 0, 2, 3).reshape(ORDER, ORDER)
        return rows.reshape(ORDER, COL_BLOCKS, col_groups, PANEL).transpose(0, 2, 1, 3).reshape(ORDER, ORDER)
    return lax.map(one_layer, jnp.arange(LAYERS, dtype=jnp.int32)).astype(jnp.float32)


def setup_inputs(seed: int = 0) -> dict:
    streams_of = jax.random.split(jax.random.key(seed), 2)
    layers = draw_layers(jax.random.fold_in(streams_of[1], 71), 0)
    return dict(layers=layers)


def to_matrix(array):
    rows = array.reshape(N_ROW, BLOCKS_DEV, PANEL, ORDER).transpose(1, 0, 2, 3).reshape(ORDER, ORDER)
    return rows.reshape(ORDER, N_COL, COL_BLOCKS, PANEL).transpose(0, 2, 1, 3).reshape(ORDER, ORDER)

def rows_to_storage(matrix):
    width = matrix.shape[1]
    return matrix.reshape(BLOCKS_DEV, N_ROW, PANEL, width).transpose(1, 0, 2, 3).reshape(ORDER, width)

def to_storage(matrix):
    rows = rows_to_storage(matrix)
    return rows.reshape(ORDER, COL_BLOCKS, N_COL, PANEL).transpose(0, 2, 1, 3).reshape(ORDER, ORDER)

def reference(layers):
    matrix = to_matrix(jnp.sum(layers, axis=0))
    identity_block = jnp.eye(PANEL, dtype=jnp.float32)
    columns = []
    for panel_step in range(PANELS):
        first = panel_step * PANEL
        after = first + PANEL
        lower_diag = jnp.linalg.cholesky(matrix[first:after, first:after])
        inverse = jax.scipy.linalg.solve_triangular(lower_diag, identity_block, lower=True)
        solved = jnp.dot(matrix[first:, first:after], inverse.T, precision=lax.Precision.HIGHEST)
        column = jnp.concatenate([jnp.zeros((first, PANEL), jnp.float32), solved], axis=0)
        columns.append(rows_to_storage(column))
        below = solved[PANEL:]
        update = jnp.dot(below, below.T, precision=lax.Precision.HIGHEST)
        matrix = matrix.at[after:, after:].add(-update)
    return (jnp.stack(columns), to_storage(matrix))
```

```python
import functools

import jax
import jax.numpy as jnp
from jax import lax
from jax.experimental import pallas as pl
from jax.experimental.pallas import tpu as pltpu
from jax.sharding import PartitionSpec as P


PANEL = 512
HALF = PANEL // 2
BASE = 16
TILE = 128
SIDE = 4
HI = lax.Precision.HIGHEST
NT = (((1,), (1,)), ((), ()))
NN = (((1,), (0,)), ((), ()))
F32 = jnp.float32
BF16 = jnp.bfloat16


def dot_full(a, b, dims):
    return lax.dot_general(a, b, dims, precision=HI, preferred_element_type=F32)


def split(a):
    high = a.astype(BF16)
    return high, (a - high.astype(F32)).astype(BF16)


def dot_split(a, b, dims):
    (a_high, a_low), (b_high, b_low) = a, b
    small = lax.dot_general(a_low, b_high, dims, preferred_element_type=F32)
    small += lax.dot_general(a_high, b_low, dims, preferred_element_type=F32)
    return small + lax.dot_general(a_high, b_high, dims, preferred_element_type=F32)


def tile_inverse(t_ref, x_ref):
    rows = lax.broadcasted_iota(jnp.int32, (TILE, TILE), 0)
    cols = lax.broadcasted_iota(jnp.int32, (TILE, TILE), 1)
    x_ref[...] = jnp.where(rows == cols, 1.0, 0.0).astype(F32)
    row_base = lax.broadcasted_iota(jnp.int32, (BASE, TILE), 0)
    for first in range(0, TILE, BASE):
        after = first + BASE
        panel = t_ref[first:after, :]
        extra = x_ref[first:after, :]
        lead = [jnp.broadcast_to(panel[:, first + k : first + k + 1], (BASE, TILE)) for k in range(BASE)]
        solved = jnp.zeros((BASE, TILE), F32)
        scale = jnp.zeros((BASE, TILE), F32)
        for j in range(BASE):
            here = row_base == j
            pivot = lead[j][j : j + 1, :]
            recip = 1.0 / pivot
            factor = jnp.where(here, 0.0, lead[j] * recip)
            extra_row = extra[j : j + 1, :]
            solved = jnp.where(here, extra_row * lax.rsqrt(pivot), solved)
            scale = jnp.where(here, recip, scale)
            for c in range(j + 1, BASE):
                lead[c] = lead[c] - factor * lead[c][j : j + 1, :]
            panel = panel - factor * panel[j : j + 1, :]
            extra = extra - factor * extra_row
        panel = panel * scale
        extra = extra * scale
        for g in range(after, TILE, 8):
            block = t_ref[g : g + 8, :]
            new = block
            other = x_ref[g : g + 8, :]
            for k in range(BASE):
                weight = jnp.broadcast_to(block[:, first + k : first + k + 1], (8, TILE))
                new = new - weight * panel[k : k + 1, :]
                other = other - weight * extra[k : k + 1, :]
            t_ref[g : g + 8, :] = new
            x_ref[g : g + 8, :] = other
        x_ref[first:after, :] = solved


def panel_inverse(t_ref, v_ref, tile_ref, inv_ref):
    v_ref[...] = jnp.zeros((PANEL, PANEL), F32)

    @pl.loop(0, PANEL // TILE)
    def _(step):
        at = pl.ds(pl.multiple_of(step * TILE, TILE), TILE)
        tile_ref[...] = t_ref[at, at]
        tile_inverse(tile_ref, inv_ref)
        for b in range(0, PANEL, TILE):

            @pl.when(step == b // TILE)
            def _():
                e = b + TILE
                x = inv_ref[...]
                if b:
                    v_ref[b:e, 0:b] = dot_full(x, v_ref[b:e, 0:b], NN)
                v_ref[b:e, b:e] = x
                if e < PANEL:
                    left = dot_full(t_ref[e:, b:e], x, NT)
                    right = dot_full(x, t_ref[b:e, e:], NN)
                    t_ref[e:, e:] = t_ref[e:, e:] - dot_full(left, right, NN)
                    v_ref[e:, 0:e] = v_ref[e:, 0:e] - dot_full(left, v_ref[b:e, 0:e], NN)


def first_kernel(a_ref, v_ref, t_ref, tile_ref, inv_ref):
    t_ref[...] = a_ref[...]
    panel_inverse(t_ref, v_ref, tile_ref, inv_ref)


def second_kernel(v0_ref, a10_ref, a11_ref, v_ref, low_ref, t_ref, tile_ref, inv_ref):
    low = dot_full(a10_ref[...], v0_ref[...], NT)
    low_ref[...] = low
    t_ref[...] = a11_ref[...] - dot_full(low, low, NT)
    panel_inverse(t_ref, v_ref, tile_ref, inv_ref)


SQUARE = jax.ShapeDtypeStruct((PANEL, PANEL), F32)


def scratch():
    return [pltpu.VMEM((PANEL, PANEL), F32), pltpu.VMEM((TILE, TILE), F32), pltpu.VMEM((TILE, TILE), F32)]


def cost(micros):
    return pl.CostEstimate(flops=int(micros * 1e9), bytes_accessed=4 << 20, transcendentals=0)


def first_inverse(a00):
    return pl.pallas_call(
        first_kernel, out_shape=SQUARE, scratch_shapes=scratch(), cost_estimate=cost(19), name="first_inverse"
    )(a00)


def second_inverse(v0, a10, a11):
    return pl.pallas_call(
        second_kernel, out_shape=(SQUARE, SQUARE), scratch_shapes=scratch(), cost_estimate=cost(23), name="second_inverse"
    )(v0, a10, a11)


def rows_kernel(place_ref, a0_ref, a1_ref, v0_ref, v1_ref, low_ref, keep_ref, send_ref, w_high, w_low, u_high, u_low):
    block = place_ref[0]
    column = place_ref[1]
    layer = place_ref[2]
    v0 = split(v0_ref[...])
    v1 = split(v1_ref[...])
    low = split(low_ref[...])
    c0 = dot_split(split(a0_ref[...]), v0, NT)
    c0_live = jnp.where(block >= 1, c0, 0.0)
    c0_parts = split(c0_live)
    rest = a1_ref[...] - dot_split(c0_parts, low, NT)
    c1 = dot_split(split(rest), v1, NT)
    c1_out = jnp.where(block >= 1, c1, 0.0)
    c1_live = jnp.where(block >= 2, c1, 0.0)
    for p, c in enumerate((c0, c1_out)):
        keep_ref[p] = jnp.where(layer == 0, c[:, :HALF], c[:, HALF:])
        send_ref[p] = jnp.where(layer == 0, c[:, HALF:], c[:, :HALF])
    w1 = dot_split(split(c1_live), v1, NN)
    alone = dot_split(c0_parts, v0, NN)
    back = dot_split(split(w1), low, NN)
    w0 = alone - dot_split(split(back), v0, NN)
    for p, (w, u) in enumerate(((w0, alone), (w1, jnp.zeros_like(w1)))):
        at = slice(p * PANEL, (p + 1) * PANEL)
        w_high[:, at], w_low[:, at] = split(w)
        u = jnp.where(column == 0, 0.0, jnp.where(column == 1, u, w))
        u_high[:, at], u_low[:, at] = split(u)


def row_phase(place, a0, a1, v0, v1, low):
    vmem = pl.BlockSpec(memory_space=pltpu.VMEM)
    half = jax.ShapeDtypeStruct((2, PANEL, HALF), F32)
    wide = jax.ShapeDtypeStruct((PANEL, 2 * PANEL), BF16)
    return pl.pallas_call(
        rows_kernel,
        in_specs=[pl.BlockSpec(memory_space=pltpu.SMEM)] + [vmem] * 5,
        out_specs=[vmem] * 6,
        out_shape=(half, half, wide, wide, wide, wide),
        cost_estimate=cost(10),
        name="row_phase",
    )(place, a0, a1, v0, v1, low)


def update_kernel(own, place_ref, mine_ref, other_ref, cols_ref, w_high, w_low, u_high, u_low, *rest):
    out_ref = rest[-1]
    first = (pl.program_id(0) == 0) & (place_ref[2] == own)
    base = mine_ref[...] + other_ref[...]
    cols = split(jnp.concatenate([cols_ref[q] for q in range(SIDE)], axis=1))

    @pl.when(first)
    def _():
        out_ref[...] = base - dot_split((u_high[...], u_low[...]), cols, NN)

    @pl.when(jnp.logical_not(first))
    def _():
        out_ref[...] = base - dot_split((w_high[...], w_low[...]), cols, NN)


def update(place, layer_part, received, cols, weights, before):
    blocks = cols.shape[0] // SIDE
    half = (lambda place: place[2]) if before is None else (lambda place: 1 - place[2])
    at = lambda i, place: (0, half(place) * blocks + i)
    weight_spec = pl.BlockSpec((PANEL, 2 * PANEL), lambda i, place: (0, 0))
    in_specs = [
        pl.BlockSpec((PANEL, PANEL), lambda i, place: (place[2], half(place) * blocks + i)),
        pl.BlockSpec((PANEL, PANEL), at),
        pl.BlockSpec((SIDE, 2 * PANEL, TILE), lambda i, place: (i, 0, 0)),
    ] + [weight_spec] * 4
    args = [layer_part, received, cols, *weights]
    aliases = {}
    if before is not None:
        in_specs.append(pl.BlockSpec(memory_space=pl.ANY))
        args.append(before)
        aliases = {8: 0}
    return pl.pallas_call(
        functools.partial(update_kernel, 0 if before is None else 1),
        grid_spec=pltpu.PrefetchScalarGridSpec(
            num_scalar_prefetch=1,
            grid=(blocks,),
            in_specs=in_specs,
            out_specs=pl.BlockSpec((PANEL, PANEL), at),
        ),
        out_shape=jax.ShapeDtypeStruct(received.shape, F32),
        input_output_aliases=aliases,
        cost_estimate=cost(9),
        name="update",
    )(place, *args)


DEPTH_SWAP = [(0, 1), (1, 0)]


def along_x(shift):
    return [(y * SIDE + x, y * SIDE + (x + shift) % SIDE) for y in range(SIDE) for x in range(SIDE)]


def along_y(shift):
    return [(y * SIDE + x, (y + shift) % SIDE * SIDE + x) for y in range(SIDE) for x in range(SIDE)]


def ring_gather(value, pairs, me, dim, after=None):
    shape = value.shape[:dim] + (SIDE,) + value.shape[dim:]
    out = jnp.zeros(shape, value.dtype)
    parts = [value] + [lax.ppermute(value, "row", pairs(k)) for k in range(1, SIDE)]
    if after is not None:
        *parts, after = lax.optimization_barrier((*parts, after()))
    for k, part in enumerate(parts):
        out = lax.dynamic_update_index_in_dim(out, part, (me - k) % SIDE, dim)
    return out if after is None else (out, after)


def depth_gather(value, me, dim):
    other = lax.ppermute(value, "depth", DEPTH_SWAP)
    pair = jnp.where(me == 0, jnp.stack((value, other), dim), jnp.stack((other, value), dim))
    return pair


def from_first_two(value, me):
    near = lax.ppermute(value, "col", [(0, 1), (1, 0)])
    straight = lax.ppermute(value, "col", [(0, 2), (1, 3)])
    crossed = lax.ppermute(value, "col", [(0, 3), (1, 2)])
    zero = jnp.where(me == 0, value, jnp.where(me == 1, near, jnp.where(me == 2, straight, crossed)))
    one = jnp.where(me == 1, value, jnp.where(me == 0, near, jnp.where(me == 2, crossed, straight)))
    return zero, one


def spread_columns(panel_rows, x, col):
    quarters = panel_rows.reshape(SIDE, TILE, PANEL).transpose(0, 2, 1)
    received = []
    for k in range(SIDE):
        pairs = []
        for y in range(SIDE):
            for s in range(SIDE):
                for source in range(2):
                    target = y * SIDE + (s + k + 2 * source) % SIDE
                    pairs.append(((y * SIDE + s) * SIDE + source, target * SIDE + s))
        piece = lax.dynamic_index_in_dim(quarters, (x + k + 2 * col) % SIDE, 0, keepdims=False)
        received.append(lax.ppermute(piece, ("row", "col"), pairs))
    received = jnp.stack(received)
    zero = lax.dynamic_index_in_dim(received, (x - col) % SIDE, 0, keepdims=False)
    one = lax.dynamic_index_in_dim(received, (x - col + 2) % SIDE, 0, keepdims=False)
    return jnp.concatenate((zero, one), axis=0)


def per_device(layers):
    row = lax.axis_index("row")
    col = lax.axis_index("col")
    depth = lax.axis_index("depth")
    x, y = row % SIDE, row // SIDE
    layer_part = layers[0]
    row_groups = lax.axis_size("row")

    mine = layer_part[:PANEL, :PANEL].reshape(2 * row_groups, BASE, PANEL)
    pieces = lax.all_to_all(mine, ("row", "depth"), 0, 0, tiled=True)
    pieces = jnp.stack((pieces[0] + pieces[1], pieces[2] + pieces[3]))

    own_panel = lax.dynamic_slice(layer_part, (depth * PANEL, 0), (PANEL, PANEL))
    panel_away = lax.dynamic_slice(layer_part, ((1 - depth) * PANEL, 0), (PANEL, PANEL))
    panel_rows = own_panel + lax.ppermute(panel_away, "depth", DEPTH_SWAP)
    away = lax.dynamic_slice(layer_part, ((1 - depth) * PANEL, 0), (PANEL, layer_part.shape[1]))
    block = depth * row_groups + row
    place = jnp.stack((block, col, depth)).astype(jnp.int32)
    pieces, away, place = lax.optimization_barrier((pieces, away, place))
    received = lax.ppermute(away, "depth", DEPTH_SWAP)

    zero, one = from_first_two(pieces, col)
    blocks = jnp.stack((zero[0], zero[1], one[1]))
    blocks, panel_rows = lax.optimization_barrier((blocks, panel_rows))
    shard = spread_columns(panel_rows, x, col)
    cols_own = lax.all_gather(shard, "row", axis=0)
    blocks = ring_gather(blocks, along_y, y, 1)
    a00 = ring_gather(blocks[0], along_x, x, 1)
    a00 = depth_gather(a00, depth, 2).reshape(PANEL, PANEL)
    others, v0 = ring_gather(blocks[1:], along_x, x, 2, lambda: first_inverse(a00))
    others = depth_gather(others, depth, 3).reshape(2, PANEL, PANEL)
    a0, a1 = from_first_two(panel_rows, col)

    v1, low = second_inverse(v0, others[0], others[1])
    keep, send, *weights = row_phase(place, a0, a1, v0, v1, low)
    cols_own, send = lax.optimization_barrier((cols_own, send))
    cols_other = lax.ppermute(cols_own, "depth", DEPTH_SWAP)
    arrived = lax.ppermute(send, "depth", DEPTH_SWAP)

    schur = update(place, layer_part, received, cols_own, weights, None)
    schur = update(place, layer_part, received, cols_other, weights, schur)
    factor = jnp.where(
        depth == 0, jnp.concatenate((keep, arrived), axis=1), jnp.concatenate((arrived, keep), axis=1)
    )
    return factor, schur


def solution(mesh):
    return jax.shard_map(
        per_device,
        mesh=mesh,
        in_specs=(P("depth", "row", "col"),),
        out_specs=(P(None, "row", "depth"), P(("row", "depth"), "col")),
        check_vma=False,
    )
```

```python
import jax
import jax.numpy as jnp
from jax import lax
from jax.experimental import pallas as pl
from jax.experimental.pallas import tpu as pltpu
from jax.sharding import PartitionSpec as P


PANEL = 512
HALF = PANEL // 2
BASE = 16
TILE = 128
SIDE = 4
HI = lax.Precision.HIGHEST
NT = (((1,), (1,)), ((), ()))
NN = (((1,), (0,)), ((), ()))
F32 = jnp.float32
BF16 = jnp.bfloat16


def dot_full(a, b, dims):
    return lax.dot_general(a, b, dims, precision=HI, preferred_element_type=F32)


def split(a):
    high = a.astype(BF16)
    return high, (a - high.astype(F32)).astype(BF16)


def dot_split(a, b, dims):
    (a_high, a_low), (b_high, b_low) = a, b
    left = jnp.concatenate((a_low, a_high, a_high), axis=dims[0][0][0])
    right = jnp.concatenate((b_high, b_low, b_high), axis=dims[0][1][0])
    return lax.dot_general(left, right, dims, preferred_element_type=F32)


def tile_inverse(t_ref, x_ref):
    rows = lax.broadcasted_iota(jnp.int32, (TILE, TILE), 0)
    cols = lax.broadcasted_iota(jnp.int32, (TILE, TILE), 1)
    x_ref[...] = jnp.where(rows == cols, 1.0, 0.0).astype(F32)
    row_base = lax.broadcasted_iota(jnp.int32, (BASE, TILE), 0)
    for first in range(0, TILE, BASE):
        after = first + BASE
        panel = t_ref[first:after, :]
        extra = x_ref[first:after, :]
        lead = [jnp.broadcast_to(panel[:, first + k : first + k + 1], (BASE, TILE)) for k in range(BASE)]
        solved = jnp.zeros((BASE, TILE), F32)
        scale = jnp.zeros((BASE, TILE), F32)
        for j in range(BASE):
            here = row_base == j
            pivot = lead[j][j : j + 1, :]
            recip = 1.0 / pivot
            factor = jnp.where(here, 0.0, lead[j] * recip)
            extra_row = extra[j : j + 1, :]
            solved = jnp.where(here, extra_row * lax.rsqrt(pivot), solved)
            scale = jnp.where(here, recip, scale)
            for c in range(j + 1, BASE):
                lead[c] = lead[c] - factor * lead[c][j : j + 1, :]
            panel = panel - factor * panel[j : j + 1, :]
            extra = extra - factor * extra_row
        panel = panel * scale
        extra = extra * scale
        for g in range(after, TILE, 8):
            block = t_ref[g : g + 8, :]
            new = block
            other = x_ref[g : g + 8, :]
            for k in range(BASE):
                weight = jnp.broadcast_to(block[:, first + k : first + k + 1], (8, TILE))
                new = new - weight * panel[k : k + 1, :]
                other = other - weight * extra[k : k + 1, :]
            t_ref[g : g + 8, :] = new
            x_ref[g : g + 8, :] = other
        x_ref[first:after, :] = solved


def panel_inverse(t_ref, v_ref, tile_ref, inv_ref):
    v_ref[...] = jnp.zeros((PANEL, PANEL), F32)

    @pl.loop(0, PANEL // TILE)
    def _(step):
        at = pl.ds(pl.multiple_of(step * TILE, TILE), TILE)
        tile_ref[...] = t_ref[at, at]
        tile_inverse(tile_ref, inv_ref)
        for b in range(0, PANEL, TILE):

            @pl.when(step == b // TILE)
            def _():
                e = b + TILE
                x = inv_ref[...]
                if b:
                    v_ref[b:e, 0:b] = dot_full(x, v_ref[b:e, 0:b], NN)
                v_ref[b:e, b:e] = x
                if e < PANEL:
                    left = dot_full(t_ref[e:, b:e], x, NT)
                    right = dot_full(x, t_ref[b:e, e:], NN)
                    t_ref[e:, e:] = t_ref[e:, e:] - dot_full(left, right, NN)
                    v_ref[e:, 0:e] = v_ref[e:, 0:e] - dot_full(left, v_ref[b:e, 0:e], NN)


def first_kernel(a_ref, v_ref, t_ref, tile_ref, inv_ref):
    t_ref[...] = a_ref[...]
    panel_inverse(t_ref, v_ref, tile_ref, inv_ref)


def second_kernel(v0_ref, a10_ref, a11_ref, v_ref, low_ref, t_ref, tile_ref, inv_ref):
    low = dot_full(a10_ref[...], v0_ref[...], NT)
    low_ref[...] = low
    t_ref[...] = a11_ref[...] - dot_full(low, low, NT)
    panel_inverse(t_ref, v_ref, tile_ref, inv_ref)


SQUARE = jax.ShapeDtypeStruct((PANEL, PANEL), F32)


def scratch():
    return [pltpu.VMEM((PANEL, PANEL), F32), pltpu.VMEM((TILE, TILE), F32), pltpu.VMEM((TILE, TILE), F32)]


def cost(micros):
    return pl.CostEstimate(flops=int(micros * 1e9), bytes_accessed=4 << 20, transcendentals=0)


def first_inverse(a00):
    return pl.pallas_call(
        first_kernel, out_shape=SQUARE, scratch_shapes=scratch(), cost_estimate=cost(19), name="first_inverse"
    )(a00)


def second_inverse(v0, a10, a11):
    return pl.pallas_call(
        second_kernel, out_shape=(SQUARE, SQUARE), scratch_shapes=scratch(), cost_estimate=cost(23), name="second_inverse"
    )(v0, a10, a11)


def rows_kernel(place_ref, a0_ref, a1_ref, v0_ref, v1_ref, low_ref, keep_ref, send_ref, w_high, w_low):
    block = place_ref[0]
    column = place_ref[1]
    layer = place_ref[2]
    v0 = split(v0_ref[...])
    v1 = split(v1_ref[...])
    low = split(low_ref[...])
    c0 = dot_split(split(a0_ref[...]), v0, NT)
    c0_live = jnp.where(block >= 1, c0, 0.0)
    c0_parts = split(c0_live)
    rest = a1_ref[...] - dot_split(c0_parts, low, NT)
    c1 = dot_split(split(rest), v1, NT)
    c1_out = jnp.where(block >= 1, c1, 0.0)
    c1_live = jnp.where(block >= 2, c1, 0.0)
    for p, c in enumerate((c0, c1_out)):
        keep_ref[p] = jnp.where(layer == 0, c[:, :HALF], c[:, HALF:])
        send_ref[p] = jnp.where(layer == 0, c[:, HALF:], c[:, :HALF])
    w1 = dot_split(split(c1_live), v1, NN)
    alone = dot_split(c0_parts, v0, NN)
    back = dot_split(split(w1), low, NN)
    w0 = alone - dot_split(split(back), v0, NN)
    for p, (w, u) in enumerate(((w0, alone), (w1, jnp.zeros_like(w1)))):
        at = slice(p * PANEL, (p + 1) * PANEL)
        w_high[0, :, at], w_low[0, :, at] = split(w)
        u = jnp.where(column == 0, 0.0, jnp.where(column == 1, u, w))
        w_high[1, :, at], w_low[1, :, at] = split(u)


def row_phase(place, a0, a1, v0, v1, low):
    whole = pl.BlockSpec((PANEL, PANEL), lambda i: (0, 0))
    part = pl.BlockSpec((TILE, PANEL), lambda i: (i, 0))
    half = jax.ShapeDtypeStruct((2, PANEL, HALF), F32)
    wide = jax.ShapeDtypeStruct((2, PANEL, 2 * PANEL), BF16)
    return pl.pallas_call(
        rows_kernel,
        grid=(PANEL // TILE,),
        in_specs=[pl.BlockSpec(memory_space=pltpu.SMEM), part, part, whole, whole, whole],
        out_specs=[pl.BlockSpec((2, TILE, HALF), lambda i: (0, i, 0))] * 2
        + [pl.BlockSpec((2, TILE, 2 * PANEL), lambda i: (0, i, 0))] * 2,
        out_shape=(half, half, wide, wide),
        cost_estimate=cost(10),
        name="row_phase",
    )(place, a0, a1, v0, v1, low)


def update_kernel(place_ref, mine_ref, other_ref, cols_ref, w_high, w_low, *rest):
    out_ref = rest[-1]
    base = mine_ref[...] + other_ref[...]
    cols = split(jnp.concatenate([cols_ref[q] for q in range(SIDE)], axis=1))
    out_ref[...] = base - dot_split((w_high[0], w_low[0]), cols, NN)


def update(place, layer_part, received, cols, weights, before):
    blocks = cols.shape[0] // SIDE
    half = (lambda place: place[2]) if before is None else (lambda place: 1 - place[2])
    at = lambda i, place: (0, half(place) * blocks + i)
    own = 0 if before is None else 1
    weight_spec = pl.BlockSpec(
        (1, PANEL, 2 * PANEL), lambda i, place: (jnp.where((i == 0) & (place[2] == own), 1, 0), 0, 0)
    )
    in_specs = [
        pl.BlockSpec((PANEL, PANEL), lambda i, place: (place[2], half(place) * blocks + i)),
        pl.BlockSpec((PANEL, PANEL), at),
        pl.BlockSpec((SIDE, 2 * PANEL, TILE), lambda i, place: (i, 0, 0)),
    ] + [weight_spec] * 2
    args = [layer_part, received, cols, *weights]
    aliases = {}
    if before is not None:
        in_specs.append(pl.BlockSpec(memory_space=pl.ANY))
        args.append(before)
        aliases = {6: 0}
    return pl.pallas_call(
        update_kernel,
        grid_spec=pltpu.PrefetchScalarGridSpec(
            num_scalar_prefetch=1,
            grid=(blocks,),
            in_specs=in_specs,
            out_specs=pl.BlockSpec((PANEL, PANEL), at),
        ),
        out_shape=jax.ShapeDtypeStruct(received.shape, F32),
        input_output_aliases=aliases,
        cost_estimate=cost(9),
        name="update",
    )(place, *args)


DEPTH_SWAP = [(0, 1), (1, 0)]


def along_x(shift):
    return [(y * SIDE + x, y * SIDE + (x + shift) % SIDE) for y in range(SIDE) for x in range(SIDE)]


def along_y(shift):
    return [(y * SIDE + x, (y + shift) % SIDE * SIDE + x) for y in range(SIDE) for x in range(SIDE)]


def ring_gather(value, pairs, me, dim, after=None):
    shape = value.shape[:dim] + (SIDE,) + value.shape[dim:]
    out = jnp.zeros(shape, value.dtype)
    parts = [value] + [lax.ppermute(value, "row", pairs(k)) for k in range(1, SIDE)]
    if after is not None:
        *parts, after = lax.optimization_barrier((*parts, after()))
    for k, part in enumerate(parts):
        out = lax.dynamic_update_index_in_dim(out, part, (me - k) % SIDE, dim)
    return out if after is None else (out, after)


def depth_gather(value, me, dim):
    other = lax.ppermute(value, "depth", DEPTH_SWAP)
    pair = jnp.where(me == 0, jnp.stack((value, other), dim), jnp.stack((other, value), dim))
    return pair


def from_first_two(value, me):
    near = lax.ppermute(value, "col", [(0, 1), (1, 0)])
    straight = lax.ppermute(value, "col", [(0, 2), (1, 3)])
    crossed = lax.ppermute(value, "col", [(0, 3), (1, 2)])
    zero = jnp.where(me == 0, value, jnp.where(me == 1, near, jnp.where(me == 2, straight, crossed)))
    one = jnp.where(me == 1, value, jnp.where(me == 0, near, jnp.where(me == 2, crossed, straight)))
    return zero, one


def spread_columns(panel_rows, x, col):
    quarters = panel_rows.reshape(SIDE, TILE, PANEL).transpose(0, 2, 1)
    received = []
    for k in range(SIDE):
        pairs = []
        for y in range(SIDE):
            for s in range(SIDE):
                for source in range(2):
                    target = y * SIDE + (s + k + 2 * source) % SIDE
                    pairs.append(((y * SIDE + s) * SIDE + source, target * SIDE + s))
        piece = lax.dynamic_index_in_dim(quarters, (x + k + 2 * col) % SIDE, 0, keepdims=False)
        received.append(lax.ppermute(piece, ("row", "col"), pairs))
    received = jnp.stack(received)
    zero = lax.dynamic_index_in_dim(received, (x - col) % SIDE, 0, keepdims=False)
    one = lax.dynamic_index_in_dim(received, (x - col + 2) % SIDE, 0, keepdims=False)
    return jnp.concatenate((zero, one), axis=0)


def per_device(layers):
    row = lax.axis_index("row")
    col = lax.axis_index("col")
    depth = lax.axis_index("depth")
    x, y = row % SIDE, row // SIDE
    layer_part = layers[0]
    row_groups = lax.axis_size("row")

    mine = layer_part[:PANEL, :PANEL].reshape(2 * row_groups, BASE, PANEL)
    pieces = lax.all_to_all(mine, ("row", "depth"), 0, 0, tiled=True)
    pieces = jnp.stack((pieces[0] + pieces[1], pieces[2] + pieces[3]))

    own_panel = lax.dynamic_slice(layer_part, (depth * PANEL, 0), (PANEL, PANEL))
    panel_away = lax.dynamic_slice(layer_part, ((1 - depth) * PANEL, 0), (PANEL, PANEL))
    panel_rows = own_panel + lax.ppermute(panel_away, "depth", DEPTH_SWAP)
    away = lax.dynamic_slice(layer_part, ((1 - depth) * PANEL, 0), (PANEL, layer_part.shape[1]))
    block = depth * row_groups + row
    place = jnp.stack((block, col, depth)).astype(jnp.int32)
    pieces, away, place = lax.optimization_barrier((pieces, away, place))
    received = lax.ppermute(away, "depth", DEPTH_SWAP)

    zero, one = from_first_two(pieces, col)
    blocks = jnp.stack((zero[0], zero[1], one[1]))
    blocks, panel_rows = lax.optimization_barrier((blocks, panel_rows))
    shard = spread_columns(panel_rows, x, col)
    cols_own = lax.all_gather(shard, "row", axis=0)
    blocks = ring_gather(blocks, along_y, y, 1)
    a00 = ring_gather(blocks[0], along_x, x, 1)
    a00 = depth_gather(a00, depth, 2).reshape(PANEL, PANEL)
    others, v0 = ring_gather(blocks[1:], along_x, x, 2, lambda: first_inverse(a00))
    others = depth_gather(others, depth, 3).reshape(2, PANEL, PANEL)
    a0, a1 = from_first_two(panel_rows, col)

    v1, low = second_inverse(v0, others[0], others[1])
    keep, send, *weights = row_phase(place, a0, a1, v0, v1, low)
    cols_own, send = lax.optimization_barrier((cols_own, send))
    cols_other = lax.ppermute(cols_own, "depth", DEPTH_SWAP)
    arrived = lax.ppermute(send, "depth", DEPTH_SWAP)

    schur = update(place, layer_part, received, cols_own, weights, None)
    schur = update(place, layer_part, received, cols_other, weights, schur)
    factor = jnp.where(
        depth == 0, jnp.concatenate((keep, arrived), axis=1), jnp.concatenate((arrived, keep), axis=1)
    )
    return factor, schur


def solution(mesh):
    return jax.shard_map(
        per_device,
        mesh=mesh,
        in_specs=(P("depth", "row", "col"),),
        out_specs=(P(None, "row", "depth"), P(("row", "depth"), "col")),
        check_vma=False,
    )
```
